32 devices in a mesh: blk: 16 (over z, x, core), grp: 2 (over y).
Axes of the slice: x: 2, y: 2, z: 4, core: 2. Of those that a mesh axis runs over, the one named last changes fastest.
Arguments:
- left_real: bfloat16 [4096, 8192], P('blk'), may hold values from -6 to 6
- left_imag: bfloat16 [4096, 8192], P('blk'), may hold values from -6 to 6
- right_real: bfloat16 [8192, 512], P('blk', 'grp'), may hold values from -0.0625 to 0.0625
- right_imag: bfloat16 [8192, 512], P('blk', 'grp'), may hold values from -0.0625 to 0.0625
- row_scale: float32 [4096], P('blk'), may hold values from 0.25 to 4
- bond_order: int32 [8192], replicated, may hold values from 0 to 8191, each once
Outputs:
- result_real: float32 [4096, 512], P('blk', 'grp')
- result_imag: float32 [4096, 512], P('blk', 'grp')
The draws below stay inside these ranges and needn't reach their ends.
Inputs may be any that keep to these rules, and one draw needn't show every extreme that they name: bond_order names each of 0 to 8191 exactly once.
All inputs are finite; a program needn't handle non-finite values.
Results may differ from the reference program's by a relative error of at most 0.0003.
Values may be sent and summed in bfloat16 or wider, within the bound.
A program may use at most 128 MiB of HBM per device.

```python
import math
import jax
import jax.numpy as jnp
from jax import lax

BOND = 8192
COLS = 512
ROWS = 4096


def levels(stream_key, extent, pieces, low, high):
    factor_of = 1.0
    for axis_at, blocks in pieces:
        heights = jax.random.uniform(jax.random.fold_in(jax.random.fold_in(stream_key, 6), axis_at), (blocks,), jnp.float32, low / len(pieces), high / len(pieces))
        factor_of = factor_of * jnp.repeat(jnp.exp(heights), extent[axis_at] // blocks).reshape((-1,) + (1,) * (len(extent) - 1 - axis_at))
    return factor_of


def normal_values(rng, shape, width, most, pieces=(), kind=jnp.bfloat16):
    drawn = width * jax.random.normal(rng, shape, jnp.float32)
    if pieces:
        drawn = drawn * levels(rng, shape, pieces, -0.22, 0.18)
    return jnp.clip(drawn, -most, most).astype(kind)


def setup_inputs(seed: int = 0) -> dict:
    splits = jax.random.split(jax.random.key(seed), 7)
    return {
        "left_real": normal_values(splits[0], (ROWS, BOND), 1.0, 6.0, ((0, 16),)),
        "left_imag": normal_values(splits[1], (ROWS, BOND), 1.0, 6.0, ((0, 16),)),
        "right_real": normal_values(splits[2], (BOND, COLS), BOND ** -0.5, 0.0625, ((0, 16), (1, 2))),
        "right_imag": normal_values(splits[3], (BOND, COLS), BOND ** -0.5, 0.0625, ((0, 16), (1, 2))),
        "row_scale": jnp.clip(jnp.exp(math.log(4.0) - 2.7725887 * jax.random.uniform(splits[4], (ROWS,), jnp.float32) ** levels(splits[4], (ROWS,), ((0, 16),), -0.2, 0.2)), 0.25, 4.0),
        "bond_order": jax.random.permutation(splits[5], BOND).astype(jnp.int32),
    }


def product(left, right):
    return jnp.dot(left.astype(jnp.float32), right.astype(jnp.float32), precision=lax.Precision.HIGHEST)

def reference(left_real, left_imag, right_real, right_imag, row_scale, bond_order):
    order = bond_order.astype(jnp.int32)
    perm_real = jnp.take(left_real, order, axis=1)
    perm_imag = jnp.take(left_imag, order, axis=1)
    raw_real = product(perm_real, right_real) - product(perm_imag, right_imag)
    raw_imag = product(perm_real, right_imag) + product(perm_imag, right_real)
    scaled_real = raw_real * row_scale[:, None]
    scaled_imag = raw_imag * row_scale[:, None]
    total = jnp.sum(scaled_real * scaled_real + scaled_imag * scaled_imag)
    factor = 1.0 / jnp.sqrt(total / jnp.float32(ROWS * COLS))
    return (scaled_real * factor, scaled_imag * factor)
```

```python
import functools

import jax
import jax.numpy as jnp
from jax import lax
from jax.experimental import pallas as pl
from jax.experimental.pallas import tpu as pltpu
from jax.sharding import PartitionSpec as P

MESH = pl.DeviceIdType.MESH
LANES = 128
GROUP = 256
PIECES = 4
STAGES = 8
UNROLL = 16


def kernel(
    devices,
    lr_hbm, li_hbm, rr_ref, ri_ref, scale_ref, order_ref,
    out_r, out_i, total_ref,
    left_v, table, picked, perm, held, acc,
    left_sem, ring_send, ring_recv, pair_send, pair_recv,
):
    rows, bond = lr_hbm.shape
    depth, cols = rr_ref.shape
    chips = devices // 2
    far = chips // 2
    per = GROUP // LANES
    words = 2 * per
    width = bond // STAGES
    piece = 2 * cols // PIECES

    me = lax.axis_index("blk")
    chip, core = me // 2, lax.rem(me, 2)
    other = 1 - core
    place = jnp.where(lax.rem(chip, 2) == 0, chip // 2, chips - 1 - chip // 2)

    def chip_at(p):
        p = lax.rem(p + 2 * chips, chips)
        return jnp.where(p < far, 2 * p, 2 * (chips - 1 - p) + 1)

    def block_at(p, which):
        return chip_at(p) * 2 + which

    partner = chip * 2 + other
    ahead = (block_at(place + 1, core), block_at(place - 1, core))

    def read_left(group, stage):
        return [
            pltpu.make_async_copy(
                src.at[pl.ds(group * GROUP, GROUP), pl.ds(stage * width, width)],
                left_v.at[n, stage],
                left_sem.at[n, stage],
            )
            for n, src in enumerate((lr_hbm, li_hbm))
        ]

    for stage in range(STAGES):
        for copy in read_left(0, stage):
            copy.start()

    barrier = pltpu.get_barrier_semaphore()
    for target in (ahead[0], ahead[1], partner):
        pl.semaphore_signal(barrier, inc=1, device_id={"blk": target}, device_id_type=MESH)

    for n, ref in enumerate((rr_ref, ri_ref)):
        held[me, n * cols:(n + 1) * cols, :] = (
            ref[...].astype(jnp.float32).T.astype(jnp.bfloat16)
        )
    acc[...] = jnp.zeros_like(acc)
    pl.semaphore_wait(barrier, 3)

    def chunk(block, c):
        return held.at[block, pl.ds(c * piece, piece), :]

    def plan(way):
        full = [(d, c) for d in range(1, far) for c in range(PIECES)]
        half = range(PIECES // 2) if way == 0 else range(PIECES // 2, PIECES)
        return full + [(far, c) for c in half]

    plans = (plan(0), plan(1))
    rounds = len(plans[0])

    def source(way, d):
        return place - d if way == 0 else place + d

    def ring_copy(way, slot, block):
        return pltpu.make_async_remote_copy(
            src_ref=chunk(block, plans[way][slot][1]),
            dst_ref=chunk(block, plans[way][slot][1]),
            send_sem=ring_send.at[way, slot],
            recv_sem=ring_recv.at[way, slot],
            device_id={"blk": ahead[way]},
            device_id_type=MESH,
        )

    def send_ring(way, slot):
        block = block_at(source(way, plans[way][slot][0] - 1), core)
        ring_copy(way, slot, block).start()

    def wait_ring(way, slot):
        block = block_at(source(way, plans[way][slot][0]), core)
        ring_copy(way, slot, block).wait_recv()

    def pair_copy(way, slot, which):
        d, c = (0, slot) if way == 2 else plans[way][slot]
        block = block_at(place if way == 2 else source(way, d), which)
        return pltpu.make_async_remote_copy(
            src_ref=chunk(block, c),
            dst_ref=chunk(block, c),
            send_sem=pair_send.at[way, slot],
            recv_sem=pair_recv.at[way, slot],
            device_id={"blk": partner},
            device_id_type=MESH,
        )

    slot_of = tuple({entry: slot for slot, entry in enumerate(p)} for p in plans)
    for slot in range(PIECES):
        for way in range(2):
            c = slot
            if (1, c) in slot_of[way]:
                send_ring(way, slot_of[way][(1, c)])
    for c in range(PIECES):
        pair_copy(2, c, core).start()

    def pass_on(slot):
        for way in range(2):
            wait_ring(way, slot)
            d, c = plans[way][slot]
            later = slot_of[way].get((d + 1, c))
            if later is not None:
                send_ring(way, later)
            pair_copy(way, slot, core).start()

    def turn(group, stage):
        for copy in read_left(group, stage):
            copy.wait()

        def step(t, _):
            at = pl.multiple_of(t * LANES, LANES)
            for n in range(2):
                for h in range(per):
                    tile = left_v[n, stage, h * LANES:(h + 1) * LANES, pl.ds(at, LANES)]
                    first = pl.multiple_of(stage * width + at, LANES)
                    table[pl.ds(first, LANES), n * per + h, :] = tile.astype(jnp.float32).T
            return 0

        lax.fori_loop(0, width // LANES, step, 0, unroll=2)

    def pick(block):
        base = block * depth

        def step(s, _):
            at = s * UNROLL
            got = []
            for u in range(UNROLL):
                got.append(table[order_ref[base + at + u]])
            for u in range(UNROLL):
                picked[at + u] = got[u]
            return 0

        lax.fori_loop(0, depth // UNROLL, step, 0)
        for w in range(words):
            perm[block, :, w * LANES:(w + 1) * LANES] = picked[:, w, :].astype(jnp.bfloat16)

    def multiply(block):
        acc[...] += jnp.dot(held[block], perm[block], preferred_element_type=jnp.float32)

    def multiply_chip(p):
        def step(which, _):
            multiply(block_at(p, which))
            return 0

        lax.fori_loop(0, 2, step, 0)

    def finish(group):
        low, high = pl.ds(0, cols), pl.ds(cols, cols)
        scale = scale_ref[:, group * GROUP:(group + 1) * GROUP]
        real = (acc[low, 0:GROUP] - acc[high, GROUP:2 * GROUP]) * scale
        imag = (acc[low, GROUP:2 * GROUP] + acc[high, 0:GROUP]) * scale
        squares = jnp.sum(real * real + imag * imag, axis=0, keepdims=True)
        total_ref[...] = squares if group == 0 else total_ref[...] + squares
        out_r[group * GROUP:(group + 1) * GROUP, :] = real.T
        out_i[group * GROUP:(group + 1) * GROUP, :] = imag.T

    def pick_some(first, last):
        lax.fori_loop(first, last, lambda b, _: (pick(b), 0)[1], 0)

    work = [functools.partial(turn, 0, s) for s in range(STAGES)]
    parts = 8
    edges = [devices * i // parts for i in range(parts + 1)]
    work += [functools.partial(pick_some, a, b) for a, b in zip(edges, edges[1:])]

    def pair_wait(d):
        for way in range(2):
            for slot, entry in enumerate(plans[way]):
                if entry[0] == d:
                    pair_copy(way, slot, other).wait_recv()

    def multiply_own():
        for c in range(PIECES):
            pair_copy(2, c, other).wait_recv()
        multiply_chip(place)

    def multiply_at(d):
        pair_wait(d)

        def step(i, _):
            side, which = i // 2, lax.rem(i, 2)
            multiply(block_at(place - d + 2 * d * side, which))
            return 0

        lax.fori_loop(0, 4 if d < far else 2, step, 0)

    work.append(multiply_own)
    early = max(1, rounds * 5 // 7)
    done = 0
    todo = list(range(1, far + 1))
    for slot in range(rounds):
        until = len(work) if slot >= early else len(work) * (slot + 1) // (early + 1)
        for item in work[done:until]:
            item()
        done = max(done, until)
        if done == len(work) and todo and todo[0] < plans[0][slot][0]:
            multiply_at(todo.pop(0))
        pass_on(slot)
    for d in todo:
        multiply_at(d)
    finish(0)

    for group in range(1, rows // GROUP):
        for stage in range(STAGES):
            for copy in read_left(group, stage):
                copy.start()
        for stage in range(STAGES):
            turn(group, stage)
        pick_some(0, devices)
        acc[...] = jnp.zeros_like(acc)
        lax.fori_loop(0, devices, lambda b, _: (multiply(b), 0)[1], 0)
        finish(group)

    for way in range(2):
        for slot in range(rounds):
            block = block_at(source(way, plans[way][slot][0] - 1), core)
            ring_copy(way, slot, block).wait_send()
            pair_copy(way, slot, core).wait_send()
    for c in range(PIECES):
        pair_copy(2, c, core).wait_send()


def body(devices, left_real, left_imag, right_real, right_imag, row_scale, bond_order):
    rows, bond = left_real.shape
    depth, cols = right_real.shape
    rounds = PIECES * devices // 4
    vmem = pl.BlockSpec(memory_space=pltpu.VMEM)
    far = pl.BlockSpec(memory_space=pl.ANY)
    words = 2 * GROUP // LANES
    out = jax.ShapeDtypeStruct((rows, cols), jnp.float32)
    real, imag, squares = pl.pallas_call(
        functools.partial(kernel, devices),
        out_shape=(out, out, jax.ShapeDtypeStruct((1, GROUP), jnp.float32)),
        in_specs=[far, far, vmem, vmem, vmem, pl.BlockSpec(memory_space=pltpu.SMEM)],
        out_specs=(vmem, vmem, vmem),
        scratch_shapes=[
            pltpu.VMEM((2, STAGES, GROUP, bond // STAGES), jnp.bfloat16),
            pltpu.VMEM((bond, words, LANES), jnp.float32),
            pltpu.VMEM((depth, words, LANES), jnp.float32),
            pltpu.VMEM((devices, depth, 2 * GROUP), jnp.bfloat16),
            pltpu.VMEM((devices, 2 * cols, depth), jnp.bfloat16),
            pltpu.VMEM((2 * cols, 2 * GROUP), jnp.float32),
            pltpu.SemaphoreType.DMA((2, STAGES)),
            pltpu.SemaphoreType.DMA((2, rounds)),
            pltpu.SemaphoreType.DMA((2, rounds)),
            pltpu.SemaphoreType.DMA((3, rounds)),
            pltpu.SemaphoreType.DMA((3, rounds)),
        ],
        compiler_params=pltpu.CompilerParams(
            collective_id=0, has_side_effects=True, vmem_limit_bytes=60 * 1024 * 1024
        ),
    )(left_real, left_imag, right_real, right_imag, row_scale.reshape(1, rows), bond_order)
    total = lax.psum(jnp.sum(squares), ("blk", "grp"))
    entries = rows * cols * lax.axis_size("blk") * lax.axis_size("grp")
    factor = 1.0 / jnp.sqrt(total / jnp.float32(entries))
    return real * factor, imag * factor


def solution(mesh):
    in_specs = (P("blk", None), P("blk", None), P("blk", "grp"), P("blk", "grp"), P("blk"), P())
    out_specs = (P("blk", "grp"), P("blk", "grp"))
    return jax.shard_map(
        functools.partial(body, mesh.shape["blk"]),
        mesh=mesh, in_specs=in_specs, out_specs=out_specs, check_vma=False,
    )
```

```python
import functools

import jax
import jax.numpy as jnp
from jax import lax
from jax.experimental import pallas as pl
from jax.experimental.pallas import tpu as pltpu
from jax.sharding import PartitionSpec as P

MESH = pl.DeviceIdType.MESH
LANES = 128
GROUP = 256
PIECES = 4
STAGES = 8
UNROLL = 16


def kernel(
    devices, groups,
    lr_hbm, li_hbm, rr_ref, ri_ref, scale_ref, order_ref,
    out_r, out_i, factor_ref,
    left_v, table, picked, perm, held, acc,
    left_sem, ring_send, ring_recv, pair_send, pair_recv,
    sums, group_sums, sum_send, sum_recv, group_send, group_recv,
):
    rows, bond = lr_hbm.shape
    depth, cols = rr_ref.shape
    chips = devices // 2
    far = chips // 2
    per = GROUP // LANES
    words = 2 * per
    width = bond // STAGES
    piece = 2 * cols // PIECES

    me = lax.axis_index("blk")
    my_group = lax.axis_index("grp")
    chip, core = me // 2, lax.rem(me, 2)
    other = 1 - core
    place = jnp.where(lax.rem(chip, 2) == 0, chip // 2, chips - 1 - chip // 2)

    def chip_at(p):
        p = lax.rem(p + 2 * chips, chips)
        return jnp.where(p < far, 2 * p, 2 * (chips - 1 - p) + 1)

    def block_at(p, which):
        return chip_at(p) * 2 + which

    partner = chip * 2 + other
    ahead = (block_at(place + 1, core), block_at(place - 1, core))

    def read_left(group, stage):
        return [
            pltpu.make_async_copy(
                src.at[pl.ds(group * GROUP, GROUP), pl.ds(stage * width, width)],
                left_v.at[n, stage],
                left_sem.at[n, stage],
            )
            for n, src in enumerate((lr_hbm, li_hbm))
        ]

    for stage in range(STAGES):
        for copy in read_left(0, stage):
            copy.start()

    barrier = pltpu.get_barrier_semaphore()
    for o in range(1, devices):
        target = lax.rem(me + o, devices)
        pl.semaphore_signal(barrier, inc=1, device_id={"blk": target}, device_id_type=MESH)
    for o in range(1, groups):
        target = lax.rem(my_group + o, groups)
        pl.semaphore_signal(barrier, inc=1, device_id={"grp": target}, device_id_type=MESH)

    for n, ref in enumerate((rr_ref, ri_ref)):
        held[me, n * cols:(n + 1) * cols, :] = (
            ref[...].astype(jnp.float32).T.astype(jnp.bfloat16)
        )
    acc[...] = jnp.zeros_like(acc)
    pl.semaphore_wait(barrier, devices + groups - 2)

    def chunk(block, c):
        return held.at[block, pl.ds(c * piece, piece), :]

    def plan(way):
        full = [(d, c) for d in range(1, far) for c in range(PIECES)]
        half = range(PIECES // 2) if way == 0 else range(PIECES // 2, PIECES)
        return full + [(far, c) for c in half]

    plans = (plan(0), plan(1))
    rounds = len(plans[0])

    def source(way, d):
        return place - d if way == 0 else place + d

    def ring_copy(way, slot, block):
        return pltpu.make_async_remote_copy(
            src_ref=chunk(block, plans[way][slot][1]),
            dst_ref=chunk(block, plans[way][slot][1]),
            send_sem=ring_send.at[way, slot],
            recv_sem=ring_recv.at[way, slot],
            device_id={"blk": ahead[way]},
            device_id_type=MESH,
        )

    def send_ring(way, slot):
        block = block_at(source(way, plans[way][slot][0] - 1), core)
        ring_copy(way, slot, block).start()

    def wait_ring(way, slot):
        block = block_at(source(way, plans[way][slot][0]), core)
        ring_copy(way, slot, block).wait_recv()

    def pair_copy(way, slot, which):
        d, c = (0, slot) if way == 2 else plans[way][slot]
        block = block_at(place if way == 2 else source(way, d), which)
        return pltpu.make_async_remote_copy(
            src_ref=chunk(block, c),
            dst_ref=chunk(block, c),
            send_sem=pair_send.at[way, slot],
            recv_sem=pair_recv.at[way, slot],
            device_id={"blk": partner},
            device_id_type=MESH,
        )

    slot_of = tuple({entry: slot for slot, entry in enumerate(p)} for p in plans)
    for slot in range(PIECES):
        for way in range(2):
            c = slot
            if (1, c) in slot_of[way]:
                send_ring(way, slot_of[way][(1, c)])
    for c in range(PIECES):
        pair_copy(2, c, core).start()

    def pass_on(slot):
        for way in range(2):
            wait_ring(way, slot)
            d, c = plans[way][slot]
            later = slot_of[way].get((d + 1, c))
            if later is not None:
                send_ring(way, later)
            pair_copy(way, slot, core).start()

    def turn(group, stage):
        for copy in read_left(group, stage):
            copy.wait()

        def step(t, _):
            at = pl.multiple_of(t * LANES, LANES)
            for n in range(2):
                for h in range(per):
                    tile = left_v[n, stage, h * LANES:(h + 1) * LANES, pl.ds(at, LANES)]
                    first = pl.multiple_of(stage * width + at, LANES)
                    table[pl.ds(first, LANES), n * per + h, :] = tile.astype(jnp.float32).T
            return 0

        lax.fori_loop(0, width // LANES, step, 0, unroll=2)

    def pick(block):
        base = block * depth

        def step(s, _):
            at = s * UNROLL
            got = []
            for u in range(UNROLL):
                got.append(table[order_ref[base + at + u]])
            for u in range(UNROLL):
                picked[pl.ds(pl.multiple_of((at + u) * words, words), words), :] = got[u]
            return 0

        lax.fori_loop(0, depth // UNROLL, step, 0)
        for w in range(words):
            perm[block, :, w * LANES:(w + 1) * LANES] = picked[
                pl.ds(w, depth, stride=words), :
            ].astype(jnp.bfloat16)

    def multiply(block):
        acc[...] += jnp.dot(held[block], perm[block], preferred_element_type=jnp.float32)

    def multiply_chip(p):
        def step(which, _):
            multiply(block_at(p, which))
            return 0

        lax.fori_loop(0, 2, step, 0)

    def sum_copy(o):
        return pltpu.make_async_remote_copy(
            src_ref=sums.at[me],
            dst_ref=sums.at[me],
            send_sem=sum_send.at[o - 1],
            recv_sem=sum_recv.at[o - 1],
            device_id={"blk": lax.rem(me + o, devices)},
            device_id_type=MESH,
        )

    def sum_wait(o):
        block = lax.rem(me + devices - o, devices)
        pltpu.make_async_remote_copy(
            src_ref=sums.at[block],
            dst_ref=sums.at[block],
            send_sem=sum_send.at[o - 1],
            recv_sem=sum_recv.at[o - 1],
            device_id={"blk": block},
            device_id_type=MESH,
        ).wait_recv()

    def group_copy(o, which):
        return pltpu.make_async_remote_copy(
            src_ref=group_sums.at[which],
            dst_ref=group_sums.at[which],
            send_sem=group_send.at[o - 1],
            recv_sem=group_recv.at[o - 1],
            device_id={"grp": lax.rem(my_group + o, groups)},
            device_id_type=MESH,
        )

    def finish(group):
        low, high = pl.ds(0, cols), pl.ds(cols, cols)
        scale = scale_ref[:, group * GROUP:(group + 1) * GROUP]
        real = (acc[low, 0:GROUP] - acc[high, GROUP:2 * GROUP]) * scale
        imag = (acc[low, GROUP:2 * GROUP] + acc[high, 0:GROUP]) * scale
        squares = jnp.sum(real * real + imag * imag, axis=0, keepdims=True)
        folded = sum(squares[:, h * LANES:(h + 1) * LANES] for h in range(per))
        sums[me] = folded if group == 0 else sums[me] + folded
        out_r[group * GROUP:(group + 1) * GROUP, :] = real.T
        if group == rows // GROUP - 1:
            for o in range(1, devices):
                sum_copy(o).start()
        out_i[group * GROUP:(group + 1) * GROUP, :] = imag.T

    def pick_some(first, last):
        lax.fori_loop(first, last, lambda b, _: (pick(b), 0)[1], 0)

    work = [functools.partial(turn, 0, s) for s in range(STAGES)]
    parts = 8
    edges = [devices * i // parts for i in range(parts + 1)]
    work += [functools.partial(pick_some, a, b) for a, b in zip(edges, edges[1:])]

    def pair_wait(d):
        for way in range(2):
            for slot, entry in enumerate(plans[way]):
                if entry[0] == d:
                    pair_copy(way, slot, other).wait_recv()

    def multiply_own():
        for c in range(PIECES):
            pair_copy(2, c, other).wait_recv()
        multiply_chip(place)

    def multiply_at(d):
        pair_wait(d)

        def step(i, _):
            side, which = i // 2, lax.rem(i, 2)
            multiply(block_at(place - d + 2 * d * side, which))
            return 0

        lax.fori_loop(0, 4 if d < far else 2, step, 0)

    work.append(multiply_own)
    early = max(1, rounds * 5 // 7)
    done = 0
    todo = list(range(1, far + 1))
    for slot in range(rounds):
        until = len(work) if slot >= early else len(work) * (slot + 1) // (early + 1)
        for item in work[done:until]:
            item()
        done = max(done, until)
        if done == len(work) and todo and todo[0] < plans[0][slot][0]:
            multiply_at(todo.pop(0))
        pass_on(slot)
    for d in todo:
        multiply_at(d)
    finish(0)

    for group in range(1, rows // GROUP):
        for stage in range(STAGES):
            for copy in read_left(group, stage):
                copy.start()
        for stage in range(STAGES):
            turn(group, stage)
        pick_some(0, devices)
        acc[...] = jnp.zeros_like(acc)
        lax.fori_loop(0, devices, lambda b, _: (multiply(b), 0)[1], 0)
        finish(group)

    for o in range(1, devices):
        sum_wait(o)
    group_sums[my_group] = jnp.sum(sums[...], axis=0)
    for way in range(2):
        for slot in range(rounds):
            block = block_at(source(way, plans[way][slot][0] - 1), core)
            ring_copy(way, slot, block).wait_send()
            pair_copy(way, slot, core).wait_send()
    for c in range(PIECES):
        pair_copy(2, c, core).wait_send()
    for o in range(1, devices):
        sum_copy(o).wait_send()
    for o in range(1, groups):
        group_copy(o, my_group).start()
    for o in range(1, groups):
        group_copy(o, lax.rem(my_group + groups - o, groups)).wait_recv()
    total = jnp.sum(jnp.sum(group_sums[...], axis=0), axis=1, keepdims=True)
    factor_ref[...] = 1.0 / jnp.sqrt(total / jnp.float32(rows * cols * devices * groups))
    for o in range(1, groups):
        group_copy(o, my_group).wait_send()


def body(devices, groups, left_real, left_imag, right_real, right_imag, row_scale, bond_order):
    rows, bond = left_real.shape
    depth, cols = right_real.shape
    rounds = PIECES * devices // 4
    vmem = pl.BlockSpec(memory_space=pltpu.VMEM)
    far = pl.BlockSpec(memory_space=pl.ANY)
    words = 2 * GROUP // LANES
    out = jax.ShapeDtypeStruct((rows, cols), jnp.float32)
    real, imag, factor = pl.pallas_call(
        functools.partial(kernel, devices, groups),
        out_shape=(out, out, jax.ShapeDtypeStruct((1, 1), jnp.float32)),
        in_specs=[far, far, vmem, vmem, vmem, pl.BlockSpec(memory_space=pltpu.SMEM)],
        out_specs=(vmem, vmem, vmem),
        scratch_shapes=[
            pltpu.VMEM((2, STAGES, GROUP, bond // STAGES), jnp.bfloat16),
            pltpu.VMEM((bond, words, LANES), jnp.float32),
            pltpu.VMEM((depth * words, LANES), jnp.float32),
            pltpu.VMEM((devices, depth, 2 * GROUP), jnp.bfloat16),
            pltpu.VMEM((devices, 2 * cols, depth), jnp.bfloat16),
            pltpu.VMEM((2 * cols, 2 * GROUP), jnp.float32),
            pltpu.SemaphoreType.DMA((2, STAGES)),
            pltpu.SemaphoreType.DMA((2, rounds)),
            pltpu.SemaphoreType.DMA((2, rounds)),
            pltpu.SemaphoreType.DMA((3, rounds)),
            pltpu.SemaphoreType.DMA((3, rounds)),
            pltpu.VMEM((devices, 1, LANES), jnp.float32),
            pltpu.VMEM((groups, 1, LANES), jnp.float32),
            pltpu.SemaphoreType.DMA((devices - 1,)),
            pltpu.SemaphoreType.DMA((devices - 1,)),
            pltpu.SemaphoreType.DMA((groups - 1,)),
            pltpu.SemaphoreType.DMA((groups - 1,)),
        ],
        compiler_params=pltpu.CompilerParams(
            collective_id=0, has_side_effects=True, vmem_limit_bytes=60 * 1024 * 1024
        ),
    )(left_real, left_imag, right_real, right_imag, row_scale.reshape(1, rows), bond_order)
    return real * factor, imag * factor


def solution(mesh):
    in_specs = (P("blk", None), P("blk", None), P("blk", "grp"), P("blk", "grp"), P("blk"), P())
    out_specs = (P("blk", "grp"), P("blk", "grp"))
    return jax.shard_map(
        functools.partial(body, mesh.shape["blk"], mesh.shape["grp"]),
        mesh=mesh, in_specs=in_specs, out_specs=out_specs, check_vma=False,
    )
```
